128 devices in a mesh: gx: 16 (over y, z), gy: 8 (over x, core).
Axes of the slice: x: 4, y: 4, z: 4, core: 2. Of those that a mesh axis runs over, the one named last changes fastest.
Arguments:
- state: float32 [8, 2, 4194304], P('gy', None, 'gx'), may hold values from -6 to 6
- fields: float32 [22], replicated, may hold values from 0.5 to 2
- couplings: float32 [22], replicated, may hold values from 0.5 to 2
- noise: float32 [8, 4, 2], P('gy'), may hold values from -5 to 5
Outputs:
- final_state: float32 [8, 2, 4194304], P('gy', None, 'gx')
- record: float32 [4, 2], replicated
The draws below stay inside these ranges and needn't reach their ends.
All inputs are finite; a program needn't handle non-finite values.
Results may differ from the reference program's by a relative error of at most 0.0001.
Values sent between devices are 32-bit elements; how exact they have to be, the bound alone decides.
A program may use at most 128 MiB of HBM per device.

```python
import math
import jax
import jax.numpy as jnp
from jax import lax

NQ = 22
STEPS = 4
TRAJ = 8
DIM = 4194304


def block_levels(rng, dims, pieces, low, top_value):
    loudness, own = 1.0, jax.random.fold_in(rng, 6)
    for dim, blocks in pieces:
        steps = jnp.exp(jax.random.uniform(jax.random.fold_in(own, dim), (blocks,), jnp.float32, low / len(pieces), top_value / len(pieces)))
        loudness = loudness * jnp.repeat(steps, dims[dim] // blocks).reshape([-1 if axis == dim else 1 for axis in range(len(dims))])
    return loudness


def bell_draw(stream_key, shape, scale, limit, shards=(), kind=jnp.bfloat16):
    gain = block_levels(stream_key, shape, shards, -0.22, 0.18) if shards else 1.0
    values = jax.random.normal(stream_key, shape, jnp.float32) * scale * gain
    return jnp.minimum(jnp.maximum(values, -limit), limit).astype(kind)


def setup_inputs(seed: int = 0) -> dict:
    key_of = jax.random.split(jax.random.key(seed), 5)
    return {
        "state": bell_draw(key_of[0], (TRAJ, 2, DIM), 1.0, 6.0, ((0, 8), (2, 16)), jnp.float32),
        "fields": jnp.clip(jnp.exp(jax.random.uniform(key_of[1], (NQ,), jnp.float32, math.log(0.5), math.log(2.0))), 0.5, 2.0),
        "couplings": jnp.clip(jnp.exp(jax.random.uniform(key_of[2], (NQ,), jnp.float32, math.log(0.5), math.log(2.0))), 0.5, 2.0),
        "noise": bell_draw(key_of[3], (TRAJ, STEPS, 2), 1.0, 5.0, ((0, 8),), jnp.float32),
    }


kappa_rate = 4.0
time_step = 0.05

def flip_qubit(amplitudes, qubit):
    shape = amplitudes.shape
    viewed = amplitudes.reshape(shape[0], shape[1], shape[2] >> qubit + 1, 2, 1 << qubit)
    return jnp.flip(viewed, 3).reshape(shape)

def reference(state, fields, couplings, noise):
    dim_total = state.shape[2]
    count_qubits = dim_total.bit_length() - 1
    position = lax.iota(jnp.int32, dim_total)
    spin_list = [1.0 - 2.0 * (position >> q & 1).astype(jnp.float32) for q in range(count_qubits)]
    occupancy = jnp.zeros((dim_total,), jnp.float32)
    energy = jnp.zeros((dim_total,), jnp.float32)
    for q in range(count_qubits):
        occupancy = occupancy + 0.5 * (1.0 - spin_list[q])
        energy = energy + couplings[q] * spin_list[q] * spin_list[(q + 1) % count_qubits]
    occupancy = occupancy / count_qubits
    amplitudes = state
    records = []
    half_root = jnp.sqrt(jnp.float32(time_step / 2.0))
    for step_id in range(noise.shape[1]):
        weight = amplitudes[:, 0] ** 2 + amplitudes[:, 1] ** 2
        norm_sum = lax.optimization_barrier(jnp.sum(weight, axis=1))
        magnet = lax.optimization_barrier(jnp.sum(weight * occupancy[None, :], axis=1)) / norm_sum
        amplitudes = amplitudes * jnp.sqrt(dim_total / norm_sum)[:, None, None]
        flipped = jnp.zeros_like(amplitudes)
        for q in range(count_qubits):
            flipped = flipped + fields[q] * flip_qubit(amplitudes, q)
        hamil = -flipped - energy[None, None, :] * amplitudes
        shift = occupancy[None, :] - magnet[:, None]
        first = (noise[:, step_id, 0] * half_root)[:, None]
        second = (noise[:, step_id, 1] * half_root)[:, None]
        real_part = amplitudes[:, 0]
        imag_part = amplitudes[:, 1]
        damping = time_step * kappa_rate * 0.5 * shift * shift
        kick = jnp.sqrt(jnp.float32(kappa_rate)) * shift
        new_real = real_part + time_step * hamil[:, 1] - damping * real_part + kick * (real_part * first - imag_part * second)
        new_imag = imag_part - time_step * hamil[:, 0] - damping * imag_part + kick * (real_part * second + imag_part * first)
        amplitudes = jnp.stack([new_real, new_imag], axis=1)
        drift = jnp.sqrt(jnp.float32(kappa_rate)) * magnet * time_step
        both = jnp.stack([drift + first[:, 0], drift + second[:, 0]], axis=1)
        records.append(lax.optimization_barrier(jnp.sum(both, axis=0)))
    return (amplitudes, jnp.stack(records))
```

```python
import functools

import jax
import jax.numpy as jnp
from jax import lax
from jax.experimental import pallas as pl
from jax.experimental.pallas import tpu as pltpu
from jax.sharding import PartitionSpec as P

MESH = pl.DeviceIdType.MESH
KAPPA = 4.0
DT = 0.05
NQ = 22
DIM = 4194304
SUBS = 4
F32 = jnp.float32


def kernel(
    fields, couplings, noise, x_ref, o_ref, rec_ref,
    bp, v1b, v1a, v2b, v2a, psi1, tee, flips, why, psi2,
    table, occ_base, en_base, scal, red_src, red_dst, rec_src, rec_dst, energies, pops,
    send_sem, recv_sem, red_send, red_recv, rec_send, rec_recv,
):
    me = lax.axis_index("gx")
    gy = lax.axis_index("gy")
    n_gx, n_gy = 16, 8

    barrier = pltpu.get_barrier_semaphore()

    def greet(k, _):
        pl.semaphore_signal(barrier, inc=1, device_id=(me ^ k, gy), device_id_type=MESH)
        return 0

    def greet_y(k, _):
        pl.semaphore_signal(barrier, inc=1, device_id=(me, gy ^ k), device_id_type=MESH)
        return 0

    lax.fori_loop(1, n_gx, greet, 0)
    lax.fori_loop(1, n_gy, greet_y, 0)

    shape3 = (8, 8, 128)
    sub = lax.broadcasted_iota(jnp.int32, (8, 128), 0)
    lane = lax.broadcasted_iota(jnp.int32, (8, 128), 1)
    even = (sub & 1) == 0
    sign = jnp.where(even, -1.0, 1.0).astype(F32)
    bit1 = (sub & 2) == 0
    even3 = jnp.broadcast_to(even[None], shape3)
    bit1_3 = jnp.broadcast_to(bit1[None], shape3)
    z0 = 1.0 - 2.0 * (lane & 1).astype(F32)

    def times_i(y):
        return sign[None] * jnp.where(even3, pltpu.roll(y, 7, 1), pltpu.roll(y, 1, 1))

    rows = lax.broadcasted_iota(jnp.int32, (128, 128), 0)
    cols = lax.broadcasted_iota(jnp.int32, (128, 128), 1)
    diff = rows ^ cols
    flip_table = jnp.zeros((128, 128), F32)
    for q in range(7):
        flip_table = jnp.where(diff == 1 << q, fields[q], flip_table)
    table[...] = flip_table
    for u in range(8):
        low = lane | ((sub >> 1) << 7) | (u << 9)
        pair = low ^ (low >> 1)
        pop = jnp.zeros((8, 128), jnp.int32)
        energy = jnp.zeros((8, 128), F32)
        for q in range(12):
            pop = pop + ((low >> q) & 1)
        for q in range(11):
            energy = energy + couplings[q] * (1.0 - 2.0 * ((pair >> q) & 1).astype(F32))
        occ_base[u] = pop.astype(F32) * (1.0 / NQ)
        en_base[u] = energy

    def fill(i, _):
        j, s = i >> 2, i & 3
        for which in range(2):
            k, d = (j, me) if which == 0 else (me, j)
            full = s | (k << 2) | (d << 6)
            pair = full ^ (full >> 1)
            total = F32(0.0)
            count = jnp.int32(0)
            for q in range(9):
                total = total + couplings[12 + q] * (1 - 2 * ((pair >> q) & 1)).astype(F32)
            for q in range(10):
                count = count + ((full >> q) & 1)
            energies[which * 64 + i] = total
            pops[which * 64 + i] = count.astype(F32) * (1.0 / NQ)
        return 0

    lax.fori_loop(0, 64, fill, 0)

    pl.semaphore_wait(barrier, n_gx - 1 + n_gy - 1)

    def send_group(src, dst, move, s):
        def one(k, _):
            other = me ^ k
            pltpu.make_async_remote_copy(
                src_ref=src.at[other, s], dst_ref=dst.at[me, s],
                send_sem=send_sem.at[move, s], recv_sem=recv_sem.at[move, s],
                device_id=(other, gy), device_id_type=MESH,
            ).start()
            return 0

        lax.fori_loop(1, n_gx, one, 0)

    def wait_bytes(ref, sem):
        pltpu.make_async_copy(ref, ref, sem).wait()

    def wait_group(dst, move, s):
        wait_bytes(dst.at[pl.ds(0, 15), s], recv_sem.at[move, s])

    def own(src, dst):
        def one(s, _):
            dst[me, s] = src[me, s]
            return 0

        lax.fori_loop(0, SUBS, one, 0)

    def reduce_send(step, norm8, mag8):
        both = jnp.concatenate(
            [jnp.sum(norm8, axis=0, keepdims=True), jnp.sum(mag8, axis=0, keepdims=True)], axis=0
        )
        red_src[step] = both
        red_dst[step, me] = both

        def one(k, _):
            pltpu.make_async_remote_copy(
                src_ref=red_src.at[step], dst_ref=red_dst.at[step, me],
                send_sem=red_send.at[step], recv_sem=red_recv.at[step],
                device_id=(me ^ k, gy), device_id_type=MESH,
            ).start()
            return 0

        lax.fori_loop(1, n_gx, one, 0)

    def reduce_wait(step):
        wait_bytes(red_dst.at[step, pl.ds(0, 15)], red_recv.at[step])
        total = jnp.sum(jnp.sum(red_dst[step], axis=0), axis=1, keepdims=True)
        norm, mag = total[0:1], total[1:2]
        scal[step, 0] = jnp.broadcast_to(mag / norm, (8, 128))
        scal[step, 1] = jnp.broadcast_to(jnp.sqrt(float(DIM) / norm), (8, 128))

    half_root = 0.15811388300841897

    def moved(step, which, index, psi, flip):
        mag, phi = scal[step, 0], scal[step, 1]
        x1 = noise[2 * step] * half_root
        x2 = noise[2 * step + 1] * half_root
        s = index & 3
        other = index >> 2
        d = me if which == 0 else other
        z12 = (1 - 2 * (s & 1)).astype(F32)
        z21 = (1 - 2 * ((d >> 3) & 1)).astype(F32)
        place = which * 64 + index
        edge = (couplings[21] * z21) * z0 + energies[place]
        off = pops[place] - mag
        turn = couplings[11] * z12
        parts = []
        for u in range(8):
            z11 = -1.0 if u & 4 else 1.0
            shift = occ_base[u] + off
            grow = phi * (1.0 + shift * (2.0 * x1 - (DT * KAPPA * 0.5) * shift))
            energy = en_base[u] + (edge + turn * z11)
            spin = phi * ((2.0 * x2) * shift + DT * energy)
            parts.append((grow, spin))
        grow = jnp.stack([p[0] for p in parts])
        spin = jnp.stack([p[1] for p in parts])
        return grow * psi + times_i(spin * psi + (DT * phi)[None] * flip)

    def weigh(index, psi, carry):
        norm8, mag8 = carry
        weight = psi * psi
        total = jnp.sum(weight, axis=0)
        part = jnp.sum(weight * occ_base[...], axis=0)
        return norm8 + total, mag8 + part + pops[index] * total

    zero8 = jnp.zeros((8, 128), F32)

    def local_flips(src, dst):
        def one(k, _):
            block = src[k]
            lanes = jnp.dot(
                block.reshape(256, 128), table[...],
                precision=lax.Precision.HIGHEST, preferred_element_type=F32,
            ).reshape(4, 8, 8, 128)
            for s in range(SUBS):
                here = block[s]
                total = lanes[s]
                total = total + fields[7] * jnp.where(
                    bit1_3, pltpu.roll(here, 6, 1), pltpu.roll(here, 2, 1)
                )
                total = total + fields[8] * pltpu.roll(here, 4, 1)
                for b in range(3):
                    total = total + fields[9 + b] * jnp.stack([here[u ^ (1 << b)] for u in range(8)])
                for b in range(2):
                    total = total + fields[12 + b] * block[s ^ (1 << b)]
                for b in range(4):
                    total = total + fields[14 + b] * src[k ^ (1 << b), s]
                dst[k, s] = total
            return 0

        lax.fori_loop(0, 16, one, 0)

    def high_flips(src, dst, s):
        def one(d, _):
            total = fields[18] * src[d ^ 1, s]
            for b in range(1, 4):
                total = total + fields[18 + b] * src[d ^ (1 << b), s]
            dst[d, s] = total
            return 0

        lax.fori_loop(0, 16, one, 0)

    def round_of(r, start, finish):
        base = 3 * r
        first, second = 2 * r, 2 * r + 1
        held, out1, in1, out2, in2 = bp.at[r], v1b.at[r], v1a.at[r], v2b.at[r], v2a.at[r]
        own(start, held)
        local_flips(start, flips)
        for s in range(SUBS):
            wait_group(held, base, s)
            high_flips(held, out1, s)
            send_group(out1, in1, base + 1, s)
        own(out1, in1)
        reduce_wait(first)
        for s in range(SUBS):

            def one(d, _):
                why[d, s] = moved(first, 1, d * 4 + s, held[d, s], out1[d, s])
                return 0

            lax.fori_loop(0, 16, one, 0)
            high_flips(why, out2, s)
            if s < 2:
                send_group(out2, in2, base + 2, s)
        own(out2, in2)
        carry = (zero8, zero8)
        for s in range(SUBS):
            wait_group(in1, base + 1, s)

            def one(k, carry):
                back = in1[k, s]
                new = moved(first, 0, k * 4 + s, start[k, s], flips[k, s] + back)
                psi1[k, s] = new
                tee[k, s] = new + times_i((DT * scal[first, 1])[None] * back)
                return weigh(k * 4 + s, new, carry)

            carry = lax.fori_loop(0, 16, one, carry)
        reduce_send(second, *carry)
        for s in range(2, SUBS):
            send_group(out2, in2, base + 2, s)
        local_flips(tee, flips)
        reduce_wait(second)
        if r == 1:
            send_record()
        carry = (zero8, zero8)
        for s in range(SUBS):
            wait_group(in2, base + 2, s)

            def one(k, carry):
                new = moved(second, 0, k * 4 + s, psi1[k, s], flips[k, s] + in2[k, s])
                finish[k, s] = new
                return weigh(k * 4 + s, new, carry) if r == 0 else carry

            carry = lax.fori_loop(0, 16, one, carry)
            if r == 0:
                send_group(finish, bp.at[1], 3, s)
        if r == 0:
            reduce_send(2, *carry)

    def send_record():
        total = zero8
        for step in range(4):
            kick = jnp.where(lane == 0, noise[2 * step], noise[2 * step + 1]) * half_root
            total = total + jnp.where(sub == step, (KAPPA ** 0.5 * DT) * scal[step, 0] + kick, 0.0)
        rec_src[...] = total
        rec_dst[gy] = total

        def one(k, _):
            pltpu.make_async_remote_copy(
                src_ref=rec_src, dst_ref=rec_dst.at[gy],
                send_sem=rec_send, recv_sem=rec_recv,
                device_id=(me, gy ^ k), device_id_type=MESH,
            ).start()
            return 0

        lax.fori_loop(1, n_gy, one, 0)

    for s in range(SUBS):
        send_group(x_ref, bp.at[0], 0, s)

    def first_weigh(i, carry):
        return weigh(i, x_ref[i >> 2, i & 3], carry)

    reduce_send(0, *lax.fori_loop(0, 64, first_weigh, (zero8, zero8)))
    round_of(0, x_ref, psi2)
    round_of(1, psi2, o_ref)

    wait_bytes(rec_dst.at[pl.ds(0, 7)], rec_recv)
    rec_ref[...] = jnp.sum(rec_dst[...], axis=0)[0:4, 0:2]

    for move in range(6):
        for s in range(SUBS):
            wait_bytes(bp.at[0, pl.ds(0, 15), s], send_sem.at[move, s])
    for step in range(4):
        wait_bytes(red_dst.at[step, pl.ds(0, 15)], red_send.at[step])
    wait_bytes(rec_dst.at[pl.ds(0, 7)], rec_send)


def shards(state, fields, couplings, noise):
    block = (16, SUBS, 8, 8, 128)
    x = state.reshape(2, 2048, 128).transpose(1, 0, 2).reshape(block)
    big = pltpu.VMEM(block, F32)
    pair = pltpu.VMEM((2, *block), F32)
    smem = pl.BlockSpec(memory_space=pltpu.SMEM)
    vmem = pl.BlockSpec(memory_space=pltpu.VMEM)
    final, record = pl.pallas_call(
        kernel,
        out_shape=(jax.ShapeDtypeStruct(block, F32), jax.ShapeDtypeStruct((4, 2), F32)),
        in_specs=[smem, smem, smem, vmem],
        out_specs=(vmem, vmem),
        scratch_shapes=[
            pair, pair, pair, pair, pair, big, big, big, big, big,
            pltpu.VMEM((128, 128), F32), pltpu.VMEM((8, 8, 128), F32), pltpu.VMEM((8, 8, 128), F32),
            pltpu.VMEM((4, 2, 8, 128), F32), pltpu.VMEM((4, 2, 128), F32), pltpu.VMEM((4, 16, 2, 128), F32),
            pltpu.VMEM((8, 128), F32), pltpu.VMEM((8, 8, 128), F32),
            pltpu.SMEM((128,), F32), pltpu.SMEM((128,), F32),
            pltpu.SemaphoreType.DMA((6, SUBS)), pltpu.SemaphoreType.DMA((6, SUBS)),
            pltpu.SemaphoreType.DMA((4,)), pltpu.SemaphoreType.DMA((4,)),
            pltpu.SemaphoreType.DMA, pltpu.SemaphoreType.DMA,
        ],
        compiler_params=pltpu.CompilerParams(
            collective_id=0, has_side_effects=True, vmem_limit_bytes=56 * 1024 * 1024
        ),
    )(fields, couplings, noise.reshape(8), x)
    final = final.reshape(2048, 2, 128).transpose(1, 0, 2).reshape(1, 2, 262144)
    return final, record


def solution(mesh):
    placed = (P("gy", None, "gx"), P(), P(), P("gy", None, None))
    return jax.shard_map(
        shards, mesh=mesh, in_specs=placed, out_specs=(P("gy", None, "gx"), P()), check_vma=False
    )
```

```python
import functools

import jax
import jax.numpy as jnp
from jax import lax
from jax.experimental import pallas as pl
from jax.experimental.pallas import tpu as pltpu
from jax.sharding import PartitionSpec as P

MESH = pl.DeviceIdType.MESH
KAPPA = 4.0
DT = 0.05
NQ = 22
DIM = 4194304
SUBS = 4
WINDOW = 4
F32 = jnp.float32


def kernel(
    fields, couplings, noise, x_hbm, o_ref, rec_ref,
    x_ref, bp, v1b, v1a, v2b, v2a, psi1, tee, flips, why, psi2,
    table, occ_base, en_base, scal, red_src, red_dst, rec_src, rec_dst, energies, pops,
    send_sem, recv_sem, red_send, red_recv, rec_send, rec_recv, load_sem,
):
    me = lax.axis_index("gx")
    gy = lax.axis_index("gy")
    n_gx, n_gy = 16, 8

    barrier = pltpu.get_barrier_semaphore()

    def greet(k, _):
        pl.semaphore_signal(barrier, inc=1, device_id=(me ^ k, gy), device_id_type=MESH)
        return 0

    def greet_y(k, _):
        pl.semaphore_signal(barrier, inc=1, device_id=(me, gy ^ k), device_id_type=MESH)
        return 0

    load = pltpu.make_async_copy(x_hbm, x_ref, load_sem)
    load.start()
    lax.fori_loop(1, n_gx, greet, 0)
    lax.fori_loop(1, n_gy, greet_y, 0)

    shape3 = (8, 8, 128)
    sub = lax.broadcasted_iota(jnp.int32, (8, 128), 0)
    lane = lax.broadcasted_iota(jnp.int32, (8, 128), 1)
    even = (sub & 1) == 0
    sign = jnp.where(even, -1.0, 1.0).astype(F32)
    bit1 = (sub & 2) == 0
    even3 = jnp.broadcast_to(even[None], shape3)
    bit1_3 = jnp.broadcast_to(bit1[None], shape3)
    z0 = 1.0 - 2.0 * (lane & 1).astype(F32)

    def times_i(y):
        return sign[None] * jnp.where(even3, pltpu.roll(y, 7, 1), pltpu.roll(y, 1, 1))

    load.wait()
    pl.semaphore_wait(barrier, n_gx - 1 + n_gy - 1)

    issued = []

    def wait_sent(move, s):
        wait_bytes(bp.at[0, pl.ds(0, 15), s], send_sem.at[move, s])

    def send_group(src, dst, move, s):
        if len(issued) >= WINDOW:
            wait_sent(*issued[-WINDOW])
        issued.append((move, s))

        def one(k, _):
            other = me ^ k
            pltpu.make_async_remote_copy(
                src_ref=src.at[other, s], dst_ref=dst.at[me, s],
                send_sem=send_sem.at[move, s], recv_sem=recv_sem.at[move, s],
                device_id=(other, gy), device_id_type=MESH,
            ).start()
            return 0

        lax.fori_loop(1, n_gx, one, 0)

    def wait_bytes(ref, sem):
        pltpu.make_async_copy(ref, ref, sem).wait()

    def wait_group(dst, move, s):
        wait_bytes(dst.at[pl.ds(0, 15), s], recv_sem.at[move, s])

    def own(src, dst):
        def one(s, _):
            dst[me, s] = src[me, s]
            return 0

        lax.fori_loop(0, SUBS, one, 0)

    def reduce_send(step, norm8, mag8):
        both = jnp.concatenate(
            [jnp.sum(norm8, axis=0, keepdims=True), jnp.sum(mag8, axis=0, keepdims=True)], axis=0
        )
        red_src[step] = both
        red_dst[step, me] = both

        def one(k, _):
            pltpu.make_async_remote_copy(
                src_ref=red_src.at[step], dst_ref=red_dst.at[step, me],
                send_sem=red_send.at[step], recv_sem=red_recv.at[step],
                device_id=(me ^ k, gy), device_id_type=MESH,
            ).start()
            return 0

        lax.fori_loop(1, n_gx, one, 0)

    def reduce_wait(step):
        wait_bytes(red_dst.at[step, pl.ds(0, 15)], red_recv.at[step])
        total = jnp.sum(jnp.sum(red_dst[step], axis=0), axis=1, keepdims=True)
        norm, mag = total[0:1], total[1:2]
        scal[step, 0] = jnp.broadcast_to(mag / norm, (8, 128))
        scal[step, 1] = jnp.broadcast_to(jnp.sqrt(float(DIM) / norm), (8, 128))

    half_root = 0.15811388300841897

    def moved(step, which, index, psi, flip):
        mag, phi = scal[step, 0], scal[step, 1]
        x1 = noise[0, step] * half_root
        x2 = noise[1, step] * half_root
        s = index & 3
        other = index >> 2
        d = me if which == 0 else other
        z12 = (1 - 2 * (s & 1)).astype(F32)
        z21 = (1 - 2 * ((d >> 3) & 1)).astype(F32)
        place = which * 64 + index
        edge = (couplings[21] * z21) * z0 + energies[place]
        off = pops[place] - mag
        turn = couplings[11] * z12
        parts = []
        for u in range(8):
            z11 = -1.0 if u & 4 else 1.0
            shift = occ_base[u] + off
            grow = phi * (1.0 + shift * (2.0 * x1 - (DT * KAPPA * 0.5) * shift))
            energy = en_base[u] + (edge + turn * z11)
            spin = phi * ((2.0 * x2) * shift + DT * energy)
            parts.append((grow, spin))
        grow = jnp.stack([p[0] for p in parts])
        spin = jnp.stack([p[1] for p in parts])
        return grow * psi + times_i(spin * psi + (DT * phi)[None] * flip)

    def weigh(index, psi, carry):
        norm8, mag8 = carry
        weight = psi * psi
        total = jnp.sum(weight, axis=0)
        part = jnp.sum(weight * occ_base[...], axis=0)
        return norm8 + total, mag8 + part + pops[index] * total

    zero8 = jnp.zeros((8, 128), F32)

    def local_flips(src, dst, lo=0, hi=16):
        def one(k, _):
            block = src[k]
            lanes = jnp.dot(
                block.reshape(256, 128), table[...],
                precision=lax.Precision.HIGHEST, preferred_element_type=F32,
            ).reshape(4, 8, 8, 128)
            for s in range(SUBS):
                here = block[s]
                total = lanes[s]
                total = total + fields[7] * jnp.where(
                    bit1_3, pltpu.roll(here, 6, 1), pltpu.roll(here, 2, 1)
                )
                total = total + fields[8] * pltpu.roll(here, 4, 1)
                for b in range(3):
                    total = total + fields[9 + b] * jnp.stack([here[u ^ (1 << b)] for u in range(8)])
                for b in range(2):
                    total = total + fields[12 + b] * block[s ^ (1 << b)]
                for b in range(4):
                    total = total + fields[14 + b] * src[k ^ (1 << b), s]
                dst[k, s] = total
            return 0

        lax.fori_loop(lo, hi, one, 0)

    def high_flips(src, dst, s):
        def one(d, _):
            total = fields[18] * src[d ^ 1, s]
            for b in range(1, 4):
                total = total + fields[18 + b] * src[d ^ (1 << b), s]
            dst[d, s] = total
            return 0

        lax.fori_loop(0, 16, one, 0)

    def round_of(r, start, finish):
        base = 3 * r
        first, second = 2 * r, 2 * r + 1
        held, out1, in1, out2, in2 = bp.at[r], v1b.at[r], v1a.at[r], v2b.at[r], v2a.at[r]
        own(start, held)
        for s in range(2):
            if r == 0:
                send_group(start, held, 0, 2 + s)
            local_flips(start, flips, 8 * s, 8 * s + 8)
        for s in range(SUBS):
            wait_group(held, base, s)
            high_flips(held, out1, s)
            send_group(out1, in1, base + 1, s)
        own(out1, in1)
        reduce_wait(first)
        for s in range(SUBS):

            def one(d, _):
                why[d, s] = moved(first, 1, d * 4 + s, held[d, s], out1[d, s])
                return 0

            lax.fori_loop(0, 16, one, 0)
            high_flips(why, out2, s)
            if s < 2:
                send_group(out2, in2, base + 2, s)
        own(out2, in2)
        carry = (zero8, zero8)
        for s in range(SUBS):
            wait_group(in1, base + 1, s)

            def one(k, carry):
                back = in1[k, s]
                new = moved(first, 0, k * 4 + s, start[k, s], flips[k, s] + back)
                psi1[k, s] = new
                tee[k, s] = new + times_i((DT * scal[first, 1])[None] * back)
                return weigh(k * 4 + s, new, carry)

            carry = lax.fori_loop(0, 16, one, carry)
        reduce_send(second, *carry)
        for s in range(2, SUBS):
            send_group(out2, in2, base + 2, s)
        local_flips(tee, flips)
        reduce_wait(second)
        if r == 1:
            send_record()

        def ready(i, _):
            k, s = i >> 2, i & 3
            psi1[k, s] = moved(second, 0, i, psi1[k, s], flips[k, s])
            return 0

        lax.fori_loop(0, 64, ready, 0)
        turn = (DT * scal[second, 1])[None]
        carry = (zero8, zero8)
        for s in range(SUBS):
            wait_group(in2, base + 2, s)

            def one(k, carry):
                new = psi1[k, s] + times_i(turn * in2[k, s])
                finish[k, s] = new
                return weigh(k * 4 + s, new, carry) if r == 0 else carry

            carry = lax.fori_loop(0, 16, one, carry)
            if r == 0:
                send_group(finish, bp.at[1], 3, s)
        if r == 0:
            reduce_send(2, *carry)

    def send_record():
        total = zero8
        for step in range(4):
            kick = jnp.where(sub == 0, noise[0, step], noise[1, step]) * half_root
            total = total + jnp.where(lane == step, (KAPPA ** 0.5 * DT) * scal[step, 0] + kick, 0.0)
        rec_src[...] = total
        rec_dst[gy] = total

        def one(k, _):
            pltpu.make_async_remote_copy(
                src_ref=rec_src, dst_ref=rec_dst.at[gy],
                send_sem=rec_send, recv_sem=rec_recv,
                device_id=(me, gy ^ k), device_id_type=MESH,
            ).start()
            return 0

        lax.fori_loop(1, n_gy, one, 0)

    for s in range(2):
        send_group(x_ref, bp.at[0], 0, s)

    rows = lax.broadcasted_iota(jnp.int32, (128, 128), 0)
    cols = lax.broadcasted_iota(jnp.int32, (128, 128), 1)
    diff = rows ^ cols
    flip_table = jnp.zeros((128, 128), F32)
    for q in range(7):
        flip_table = jnp.where(diff == 1 << q, fields[q], flip_table)
    table[...] = flip_table
    for u in range(8):
        low = lane | ((sub >> 1) << 7) | (u << 9)
        pair = low ^ (low >> 1)
        pop = jnp.zeros((8, 128), jnp.int32)
        energy = jnp.zeros((8, 128), F32)
        for q in range(12):
            pop = pop + ((low >> q) & 1)
        for q in range(11):
            energy = energy + couplings[q] * (1.0 - 2.0 * ((pair >> q) & 1).astype(F32))
        occ_base[u] = pop.astype(F32) * (1.0 / NQ)
        en_base[u] = energy

    def fill(i, _):
        j, s = i >> 2, i & 3
        for which in range(2):
            k, d = (j, me) if which == 0 else (me, j)
            full = s | (k << 2) | (d << 6)
            pair = full ^ (full >> 1)
            total = F32(0.0)
            count = jnp.int32(0)
            for q in range(9):
                total = total + couplings[12 + q] * (1 - 2 * ((pair >> q) & 1)).astype(F32)
            for q in range(10):
                count = count + ((full >> q) & 1)
            energies[which * 64 + i] = total
            pops[which * 64 + i] = count.astype(F32) * (1.0 / NQ)
        return 0

    lax.fori_loop(0, 64, fill, 0)

    def first_weigh(i, carry):
        return weigh(i, x_ref[i >> 2, i & 3], carry)

    reduce_send(0, *lax.fori_loop(0, 64, first_weigh, (zero8, zero8)))
    round_of(0, x_ref, psi2)
    round_of(1, psi2, o_ref)

    wait_bytes(rec_dst.at[pl.ds(0, 7)], rec_recv)
    rec_ref[...] = jnp.sum(rec_dst[...], axis=0)[0:2, 0:4]

    for pair in issued[-WINDOW:]:
        wait_sent(*pair)
    for step in range(4):
        wait_bytes(red_dst.at[step, pl.ds(0, 15)], red_send.at[step])
    wait_bytes(rec_dst.at[pl.ds(0, 7)], rec_send)


def shards(state, fields, couplings, noise):
    block = (16, SUBS, 8, 8, 128)
    x = state.reshape(2, 2048, 128).transpose(1, 0, 2).reshape(block)
    big = pltpu.VMEM(block, F32)
    pair = pltpu.VMEM((2, *block), F32)
    smem = pl.BlockSpec(memory_space=pltpu.SMEM)
    vmem = pl.BlockSpec(memory_space=pltpu.VMEM)
    final, record = pl.pallas_call(
        kernel,
        out_shape=(pltpu.VMEM(block, F32), pltpu.VMEM((2, 4), F32)),
        in_specs=[smem, smem, smem, pl.BlockSpec(memory_space=pl.ANY)],
        out_specs=(vmem, vmem),
        scratch_shapes=[
            big, pair, pair, pair, pair, pair, big, big, big, big, big,
            pltpu.VMEM((128, 128), F32), pltpu.VMEM((8, 8, 128), F32), pltpu.VMEM((8, 8, 128), F32),
            pltpu.VMEM((4, 2, 8, 128), F32), pltpu.VMEM((4, 2, 128), F32), pltpu.VMEM((4, 16, 2, 128), F32),
            pltpu.VMEM((8, 128), F32), pltpu.VMEM((8, 8, 128), F32),
            pltpu.SMEM((128,), F32), pltpu.SMEM((128,), F32),
            pltpu.SemaphoreType.DMA((6, SUBS)), pltpu.SemaphoreType.DMA((6, SUBS)),
            pltpu.SemaphoreType.DMA((4,)), pltpu.SemaphoreType.DMA((4,)),
            pltpu.SemaphoreType.DMA, pltpu.SemaphoreType.DMA, pltpu.SemaphoreType.DMA,
        ],
        compiler_params=pltpu.CompilerParams(
            collective_id=0, has_side_effects=True, vmem_limit_bytes=56 * 1024 * 1024
        ),
    )(fields, couplings, noise.transpose(0, 2, 1).reshape(2, 4), x)
    final = final.reshape(2048, 2, 128).transpose(1, 0, 2).reshape(1, 2, 262144)
    return final, record.transpose(1, 0)


def solution(mesh):
    placed = (P("gy", None, "gx"), P(), P(), P("gy", None, None))
    return jax.shard_map(
        shards, mesh=mesh, in_specs=placed, out_specs=(P("gy", None, "gx"), P()), check_vma=False
    )
```

```python
import functools

import jax
import jax.numpy as jnp
from jax import lax
from jax.experimental import pallas as pl
from jax.experimental.pallas import tpu as pltpu
from jax.sharding import PartitionSpec as P

MESH = pl.DeviceIdType.MESH
KAPPA = 4.0
DT = 0.05
NQ = 22
DIM = 4194304
SUBS = 8
F32 = jnp.float32


def kernel(
    fields, couplings, noise, x_hbm, o_ref, rec_ref,
    x_ref, bp, v1b, v1a, v2b, v2a, psi1, tee, flips, why, psi2,
    table, occ_base, en_base, scal, red_src, red_dst, rec_src, rec_dst, parts, energies, pops,
    send_sem, recv_sem, red_send, red_recv, rec_send, rec_recv, load_sem,
):
    me = lax.axis_index("gx")
    gy = lax.axis_index("gy")
    n_gx, n_gy = 16, 8

    barrier = pltpu.get_barrier_semaphore()

    def greet(k, _):
        pl.semaphore_signal(barrier, inc=1, device_id=(me ^ k, gy), device_id_type=MESH)
        return 0

    def greet_y(k, _):
        pl.semaphore_signal(barrier, inc=1, device_id=(me, gy ^ k), device_id_type=MESH)
        return 0

    load = pltpu.make_async_copy(x_hbm, x_ref, load_sem)
    load.start()
    lax.fori_loop(1, n_gx, greet, 0)
    lax.fori_loop(1, n_gy, greet_y, 0)

    shape3 = (4, 8, 128)
    sub = lax.broadcasted_iota(jnp.int32, (8, 128), 0)
    lane = lax.broadcasted_iota(jnp.int32, (8, 128), 1)
    even = (sub & 1) == 0
    sign = jnp.where(even, -1.0, 1.0).astype(F32)
    bit1 = (sub & 2) == 0
    even3 = jnp.broadcast_to(even[None], shape3)
    bit1_3 = jnp.broadcast_to(bit1[None], shape3)
    z0 = 1.0 - 2.0 * (lane & 1).astype(F32)

    def times_i(y):
        return sign[None] * jnp.where(even3, pltpu.roll(y, 7, 1), pltpu.roll(y, 1, 1))

    load.wait()
    pl.semaphore_wait(barrier, n_gx - 1 + n_gy - 1)

    def partner_mask(s):
        t = s & 3
        return (1 + 2 * (t >> 1)) * (4 - 3 * (t & 1))

    def near_mask(s, i):
        t = s & 3
        return (i >> 2) * (3 - 2 * (t >> 1)) * (4 - 3 * (t & 1)) + (i & 3) * (1 + 3 * (t & 1))

    def start_copy(src, dst, move, s, other):
        pltpu.make_async_remote_copy(
            src_ref=src, dst_ref=dst, send_sem=send_sem.at[move, s], recv_sem=recv_sem.at[move, s],
            device_id=(other, gy), device_id_type=MESH,
        ).start()

    def wait_bytes(ref, sem):
        pltpu.make_async_copy(ref, ref, sem).wait()

    def wait_group(move, s, count=14):
        wait_bytes(bp.at[0, 0, pl.ds(0, count), s], recv_sem.at[move, s])

    def send_direct(src, dst, move, s):
        pm = partner_mask(s)
        partner = me ^ pm

        def one(i, _):
            other = me ^ near_mask(s, i)
            start_copy(src.at[other, s], dst.at[0, me, s], move, s, other)
            start_copy(src.at[other ^ pm, s], dst.at[1, me, s], move, s, other)
            return 0

        lax.fori_loop(1, 8, one, 0)
        start_copy(src.at[partner, s], dst.at[0, me, s], move + 1, s, partner)
        start_copy(src.at[me, s], dst.at[1, me, s], move + 1, s, partner)

    def relay(held, move, s):
        partner = me ^ partner_mask(s)

        def one(i, _):
            source = me ^ near_mask(s, i)
            start_copy(held.at[0, source, s], held.at[1, source, s], move + 1, s, partner)
            start_copy(held.at[1, source, s], held.at[0, source, s], move + 1, s, partner)
            return 0

        lax.fori_loop(1, 8, one, 0)

    def send_back(src, dst, move, s):
        pm = partner_mask(s)

        def one(i, _):
            other = me ^ near_mask(s, i)
            start_copy(src.at[0, other, s], dst.at[me, s], move, s, other)
            start_copy(src.at[1, other, s], dst.at[me ^ pm, s], move, s, other)
            return 0

        lax.fori_loop(1, 8, one, 0)

    def keep_own(src, dst):
        def one(s, _):
            dst[0, me, s] = src[me, s]
            dst[1, me, s] = src[me ^ partner_mask(s), s]
            return 0

        lax.fori_loop(0, SUBS, one, 0)

    def take_own(src, dst):
        def one(s, _):
            dst[me, s] = src[0, me, s]
            dst[me ^ partner_mask(s), s] = src[1, me, s]
            return 0

        lax.fori_loop(0, SUBS, one, 0)

    def reduce_send(step, norm8, mag8):
        both = jnp.concatenate(
            [jnp.sum(norm8, axis=0, keepdims=True), jnp.sum(mag8, axis=0, keepdims=True)], axis=0
        )
        red_src[step] = both
        red_dst[step, me] = both

        def one(k, _):
            pltpu.make_async_remote_copy(
                src_ref=red_src.at[step], dst_ref=red_dst.at[step, me],
                send_sem=red_send.at[step], recv_sem=red_recv.at[step],
                device_id=(me ^ k, gy), device_id_type=MESH,
            ).start()
            return 0

        lax.fori_loop(1, n_gx, one, 0)

    def reduce_wait(step):
        wait_bytes(red_dst.at[step, pl.ds(0, 15)], red_recv.at[step])
        total = jnp.sum(jnp.sum(red_dst[step], axis=0), axis=1, keepdims=True)
        norm, mag = total[0:1], total[1:2]
        scal[step, 0] = jnp.broadcast_to(mag / norm, (8, 128))
        scal[step, 1] = jnp.broadcast_to(jnp.sqrt(float(DIM) / norm), (8, 128))

    half_root = 0.15811388300841897

    def moved(step, which, j, s, psi, flip):
        mag, phi = scal[step, 0], scal[step, 1]
        x1 = noise[0, step] * half_root
        x2 = noise[1, step] * half_root
        d = me if which == 0 else j
        z11 = 1.0 - 2.0 * (s & 1)
        z21 = (1 - 2 * ((d >> 3) & 1)).astype(F32)
        place = which * 128 + j * 8 + s
        edge = (couplings[21] * z21) * z0 + energies[place]
        off = pops[place] - mag
        turn = couplings[10] * z11
        grows, spins = [], []
        for u in range(4):
            z10 = -1.0 if u & 2 else 1.0
            shift = occ_base[u] + off
            grows.append(phi * (1.0 + shift * (2.0 * x1 - (DT * KAPPA * 0.5) * shift)))
            energy = en_base[u] + (edge + turn * z10)
            spins.append(phi * ((2.0 * x2) * shift + DT * energy))
        return jnp.stack(grows) * psi + times_i(jnp.stack(spins) * psi + (DT * phi)[None] * flip)

    def weigh(index, psi, carry):
        norm8, mag8 = carry
        weight = psi * psi
        total = jnp.sum(weight, axis=0)
        part = jnp.sum(weight * occ_base[...], axis=0)
        return norm8 + total, mag8 + part + pops[index] * total

    zero8 = jnp.zeros((8, 128), F32)

    def local_flips(src, dst, lo=0, hi=16):
        def one(k, _):
            block = src[k]
            lanes = jnp.dot(
                block.reshape(256, 128), table[...],
                precision=lax.Precision.HIGHEST, preferred_element_type=F32,
            ).reshape(SUBS, 4, 8, 128)
            for s in range(SUBS):
                here = block[s]
                total = lanes[s]
                total = total + fields[7] * jnp.where(
                    bit1_3, pltpu.roll(here, 6, 1), pltpu.roll(here, 2, 1)
                )
                total = total + fields[8] * pltpu.roll(here, 4, 1)
                for b in range(2):
                    total = total + fields[9 + b] * jnp.stack([here[u ^ (1 << b)] for u in range(4)])
                for b in range(3):
                    total = total + fields[11 + b] * block[s ^ (1 << b)]
                for b in range(4):
                    total = total + fields[14 + b] * src[k ^ (1 << b), s]
                dst[k, s] = total
            return 0

        lax.fori_loop(lo, hi, one, 0)

    def high_flip(src, side, d, s):
        total = fields[18] * src[side, d ^ 1, s]
        for b in range(1, 4):
            total = total + fields[18 + b] * src[side, d ^ (1 << b), s]
        return total

    def round_of(r, start, finish):
        base = 4 * r
        first, second = 2 * r, 2 * r + 1
        held, out1, in1, out2, in2 = bp.at[r], v1b.at[r], v1a.at[r], v2b.at[r], v2a.at[r]
        keep_own(start, held)
        for part in range(4):
            for s in range(2 * part, 2 * part + 2):
                wait_group(base, s)
                relay(held, base, s)
            local_flips(start, flips, 4 * part, 4 * part + 4)
        for s in range(SUBS):
            wait_group(base + 1, s, 16)

            def one(d, _):
                for side in range(2):
                    out1[side, d, s] = high_flip(held, side, d, s)
                return 0

            lax.fori_loop(0, 16, one, 0)
            send_back(out1, in1, base + 2, s)
        take_own(out1, in1)
        reduce_wait(first)
        for s in range(SUBS):

            def one(d, _):
                for side in range(2):
                    why[side, d, s] = moved(first, 1 + side, d, s, held[side, d, s], out1[side, d, s])
                return 0

            lax.fori_loop(0, 16, one, 0)

            def two(i, _):
                d = me ^ near_mask(s, i)
                for side in range(2):
                    out2[side, d, s] = high_flip(why, side, d, s)
                return 0

            lax.fori_loop(0, 8, two, 0)
            if s < SUBS // 2:
                send_back(out2, in2, base + 3, s)
        take_own(out2, in2)
        carry = (zero8, zero8)
        for s in range(SUBS):
            wait_group(base + 2, s)

            def one(k, carry):
                back = in1[k, s]
                new = moved(first, 0, k, s, start[k, s], flips[k, s] + back)
                psi1[k, s] = new
                tee[k, s] = new + times_i((DT * scal[first, 1])[None] * back)
                return weigh(k * 8 + s, new, carry)

            carry = lax.fori_loop(0, 16, one, carry)
        reduce_send(second, *carry)
        for s in range(SUBS // 2, SUBS):
            send_back(out2, in2, base + 3, s)
        local_flips(tee, flips)
        reduce_wait(second)
        if r == 0:
            carry = (zero8, zero8)
            for s in range(SUBS):
                wait_group(base + 3, s)

                def one(k, carry):
                    new = moved(second, 0, k, s, psi1[k, s], flips[k, s] + in2[k, s])
                    finish[k, s] = new
                    return weigh(k * 8 + s, new, carry)

                carry = lax.fori_loop(0, 16, one, carry)
                send_direct(finish, bp.at[1], 4, s)
            reduce_send(2, *carry)
        else:
            send_record()
            for s in range(SUBS):

                def one(k, _):
                    psi1[k, s] = moved(second, 0, k, s, psi1[k, s], flips[k, s])
                    return 0

                lax.fori_loop(0, 16, one, 0)
            turn = (DT * scal[second, 1])[None]
            for s in range(SUBS):
                wait_group(base + 3, s)

                def one(k, _):
                    finish[k, s] = psi1[k, s] + times_i(turn * in2[k, s])
                    return 0

                lax.fori_loop(0, 16, one, 0)

    def send_record():
        total = zero8
        for step in range(4):
            kick = jnp.where(sub == 0, noise[0, step], noise[1, step]) * half_root
            total = total + jnp.where(lane == step, (KAPPA ** 0.5 * DT) * scal[step, 0] + kick, 0.0)
        rec_src[...] = total
        rec_dst[gy] = total

        def one(k, _):
            pltpu.make_async_remote_copy(
                src_ref=rec_src, dst_ref=rec_dst.at[gy],
                send_sem=rec_send, recv_sem=rec_recv,
                device_id=(me, gy ^ k), device_id_type=MESH,
            ).start()
            return 0

        lax.fori_loop(1, n_gy, one, 0)

    for s in range(SUBS):
        send_direct(x_ref, bp.at[0], 0, s)

    rows = lax.broadcasted_iota(jnp.int32, (128, 128), 0)
    cols = lax.broadcasted_iota(jnp.int32, (128, 128), 1)
    diff = rows ^ cols
    flip_table = jnp.zeros((128, 128), F32)
    for q in range(7):
        flip_table = jnp.where(diff == 1 << q, fields[q], flip_table)
    table[...] = flip_table
    for u in range(4):
        low = lane | ((sub >> 1) << 7) | (u << 9)
        pair = low ^ (low >> 1)
        pop = jnp.zeros((8, 128), jnp.int32)
        energy = jnp.zeros((8, 128), F32)
        for q in range(11):
            pop = pop + ((low >> q) & 1)
        for q in range(10):
            energy = energy + couplings[q] * (1.0 - 2.0 * ((pair >> q) & 1).astype(F32))
        occ_base[u] = pop.astype(F32) * (1.0 / NQ)
        en_base[u] = energy

    def spin(number, bit):
        return (1 - 2 * ((number >> bit) & 1)).astype(F32)

    def fill_parts(i, _):
        pair = i ^ (i >> 1)
        parts[i] = couplings[11] * spin(pair, 0) + couplings[12] * spin(pair, 1)
        for first, at in ((14, 16), (18, 32)):
            total = couplings[first] * spin(pair, 0)
            for b in range(1, 3):
                total = total + couplings[first + b] * spin(pair, b)
            parts[at + i] = total
        count = (i & 1) + ((i >> 1) & 1) + ((i >> 2) & 1) + ((i >> 3) & 1)
        parts[48 + i] = count.astype(F32) * (1.0 / NQ)
        return 0

    lax.fori_loop(0, 16, fill_parts, 0)

    def fill(i, _):
        j, s = i >> 3, i & 7
        for which, k, d in ((0, j, me), (1, me, j), (2, me ^ partner_mask(s), j)):
            energies[which * 128 + i] = (
                parts[s] + parts[16 + k] + parts[32 + d]
                + couplings[13] * spin((s >> 2) ^ k, 0) + couplings[17] * spin((k >> 3) ^ d, 0)
            )
            pops[which * 128 + i] = parts[48 + s] + parts[48 + k] + parts[48 + d]
        return 0

    lax.fori_loop(0, 128, fill, 0)

    def first_weigh(i, carry):
        return weigh(i, x_ref[i >> 3, i & 7], carry)

    reduce_send(0, *lax.fori_loop(0, 128, first_weigh, (zero8, zero8)))
    round_of(0, x_ref, psi2)
    round_of(1, psi2, o_ref)

    wait_bytes(rec_dst.at[pl.ds(0, 7)], rec_recv)
    rec_ref[...] = jnp.sum(rec_dst[...], axis=0)[0:2, 0:4]

    for move in range(8):
        for s in range(SUBS):
            count = 16 if move % 4 == 1 else 14
            wait_bytes(bp.at[0, 0, pl.ds(0, count), s], send_sem.at[move, s])
    for step in range(4):
        wait_bytes(red_dst.at[step, pl.ds(0, 15)], red_send.at[step])
    wait_bytes(rec_dst.at[pl.ds(0, 7)], rec_send)


def shards(state, fields, couplings, noise):
    block = (16, SUBS, 4, 8, 128)
    x = state.reshape(2, 2048, 128).transpose(1, 0, 2).reshape(block)
    big = pltpu.VMEM(block, F32)
    pair = pltpu.VMEM((2, *block), F32)
    twin = pltpu.VMEM((2, 2, *block), F32)
    smem = pl.BlockSpec(memory_space=pltpu.SMEM)
    vmem = pl.BlockSpec(memory_space=pltpu.VMEM)
    final, record = pl.pallas_call(
        kernel,
        out_shape=(pltpu.VMEM(block, F32), pltpu.VMEM((2, 4), F32)),
        in_specs=[smem, smem, smem, pl.BlockSpec(memory_space=pl.ANY)],
        out_specs=(vmem, vmem),
        scratch_shapes=[
            big, twin, twin, pair, twin, pair, big, big, big, pair, big,
            pltpu.VMEM((128, 128), F32), pltpu.VMEM((4, 8, 128), F32), pltpu.VMEM((4, 8, 128), F32),
            pltpu.VMEM((4, 2, 8, 128), F32), pltpu.VMEM((4, 2, 128), F32), pltpu.VMEM((4, 16, 2, 128), F32),
            pltpu.VMEM((8, 128), F32), pltpu.VMEM((8, 8, 128), F32),
            pltpu.SMEM((64,), F32), pltpu.SMEM((384,), F32), pltpu.SMEM((384,), F32),
            pltpu.SemaphoreType.DMA((8, SUBS)), pltpu.SemaphoreType.DMA((8, SUBS)),
            pltpu.SemaphoreType.DMA((4,)), pltpu.SemaphoreType.DMA((4,)),
            pltpu.SemaphoreType.DMA, pltpu.SemaphoreType.DMA, pltpu.SemaphoreType.DMA,
        ],
        compiler_params=pltpu.CompilerParams(
            collective_id=0, has_side_effects=True, vmem_limit_bytes=60 * 1024 * 1024
        ),
    )(fields, couplings, noise.transpose(0, 2, 1).reshape(2, 4), x)
    final = final.reshape(2048, 2, 128).transpose(1, 0, 2).reshape(1, 2, 262144)
    return final, record.transpose(1, 0)


def solution(mesh):
    placed = (P("gy", None, "gx"), P(), P(), P("gy", None, None))
    return jax.shard_map(
        shards, mesh=mesh, in_specs=placed, out_specs=(P("gy", None, "gx"), P()), check_vma=False
    )
```

```python
import functools

import jax
import jax.numpy as jnp
from jax import lax
from jax.experimental import pallas as pl
from jax.experimental.pallas import tpu as pltpu
from jax.sharding import PartitionSpec as P

MESH = pl.DeviceIdType.MESH
KAPPA = 4.0
DT = 0.05
NQ = 22
DIM = 4194304
SUBS = 8
F32 = jnp.float32


def kernel(
    fields, couplings, noise, x_hbm, o_ref, rec_ref,
    x_ref, bp, v1b, v1a, v2b, v2a, psi1, tee, flips, why, psi2,
    table, occ_base, en_base, scal, red_src, red_dst, rec_src, rec_dst, parts, energies, pops,
    send_sem, recv_sem, red_send, red_recv, rec_send, rec_recv, load_sem,
):
    me = lax.axis_index("gx")
    gy = lax.axis_index("gy")
    n_gx, n_gy = 16, 8

    barrier = pltpu.get_barrier_semaphore()

    def greet(k, _):
        pl.semaphore_signal(barrier, inc=1, device_id=(me ^ k, gy), device_id_type=MESH)
        return 0

    def greet_y(k, _):
        pl.semaphore_signal(barrier, inc=1, device_id=(me, gy ^ k), device_id_type=MESH)
        return 0

    load = pltpu.make_async_copy(x_hbm, x_ref, load_sem)
    load.start()
    lax.fori_loop(1, n_gx, greet, 0)
    lax.fori_loop(1, n_gy, greet_y, 0)

    shape3 = (4, 8, 128)
    sub = lax.broadcasted_iota(jnp.int32, (8, 128), 0)
    lane = lax.broadcasted_iota(jnp.int32, (8, 128), 1)
    even = (sub & 1) == 0
    sign = jnp.where(even, -1.0, 1.0).astype(F32)
    bit1 = (sub & 2) == 0
    even3 = jnp.broadcast_to(even[None], shape3)
    bit1_3 = jnp.broadcast_to(bit1[None], shape3)
    z0 = 1.0 - 2.0 * (lane & 1).astype(F32)

    def times_i(y):
        return sign[None] * jnp.where(even3, pltpu.roll(y, 7, 1), pltpu.roll(y, 1, 1))

    load.wait()
    pl.semaphore_wait(barrier, n_gx - 1 + n_gy - 1)

    def partner_mask(s):
        t = s & 3
        return (1 + 2 * (t >> 1)) * (4 - 3 * (t & 1))

    def near_mask(s, i):
        t = s & 3
        return (i >> 2) * (3 - 2 * (t >> 1)) * (4 - 3 * (t & 1)) + (i & 3) * (1 + 3 * (t & 1))

    def start_copy(src, dst, move, s, other):
        pltpu.make_async_remote_copy(
            src_ref=src, dst_ref=dst, send_sem=send_sem.at[move, s], recv_sem=recv_sem.at[move, s],
            device_id=(other, gy), device_id_type=MESH,
        ).start()

    def wait_bytes(ref, sem):
        pltpu.make_async_copy(ref, ref, sem).wait()

    def wait_group(move, s, count=14):
        wait_bytes(bp.at[0, 0, pl.ds(0, count), s], recv_sem.at[move, s])

    def send_direct(src, dst, move, s):
        pm = partner_mask(s)
        partner = me ^ pm

        def one(i, _):
            other = me ^ near_mask(s, i)
            start_copy(src.at[other, s], dst.at[0, me, s], move, s, other)
            start_copy(src.at[other ^ pm, s], dst.at[1, me, s], move, s, other)
            return 0

        lax.fori_loop(1, 8, one, 0)
        start_copy(src.at[partner, s], dst.at[0, me, s], move + 1, s, partner)
        start_copy(src.at[me, s], dst.at[1, me, s], move + 1, s, partner)

    def relay(held, move, s):
        partner = me ^ partner_mask(s)

        def one(i, _):
            source = me ^ near_mask(s, i)
            start_copy(held.at[0, source, s], held.at[1, source, s], move + 1, s, partner)
            start_copy(held.at[1, source, s], held.at[0, source, s], move + 1, s, partner)
            return 0

        lax.fori_loop(1, 8, one, 0)

    def send_back(src, dst, move, s):
        pm = partner_mask(s)

        def one(i, _):
            other = me ^ near_mask(s, i)
            start_copy(src.at[0, other, s], dst.at[me, s], move, s, other)
            start_copy(src.at[1, other, s], dst.at[me ^ pm, s], move, s, other)
            return 0

        lax.fori_loop(1, 8, one, 0)

    def keep_own(src, dst):
        def one(s, _):
            dst[0, me, s] = src[me, s]
            dst[1, me, s] = src[me ^ partner_mask(s), s]
            return 0

        lax.fori_loop(0, SUBS, one, 0)

    def take_own(src, dst):
        def one(s, _):
            dst[me, s] = src[0, me, s]
            dst[me ^ partner_mask(s), s] = src[1, me, s]
            return 0

        lax.fori_loop(0, SUBS, one, 0)

    def reduce_send(step, norm8, mag8):
        both = jnp.concatenate(
            [jnp.sum(norm8, axis=0, keepdims=True), jnp.sum(mag8, axis=0, keepdims=True)], axis=0
        )
        red_src[step] = both
        red_dst[step, me] = both

        def one(k, _):
            pltpu.make_async_remote_copy(
                src_ref=red_src.at[step], dst_ref=red_dst.at[step, me],
                send_sem=red_send.at[step], recv_sem=red_recv.at[step],
                device_id=(me ^ k, gy), device_id_type=MESH,
            ).start()
            return 0

        lax.fori_loop(1, n_gx, one, 0)

    def reduce_wait(step):
        wait_bytes(red_dst.at[step, pl.ds(0, 15)], red_recv.at[step])
        total = jnp.sum(jnp.sum(red_dst[step], axis=0), axis=1, keepdims=True)
        norm, mag = total[0:1], total[1:2]
        scal[step, 0] = jnp.broadcast_to(mag / norm, (8, 128))
        scal[step, 1] = jnp.broadcast_to(jnp.sqrt(float(DIM) / norm), (8, 128))

    half_root = 0.15811388300841897

    def moved(step, which, j, s, psi, flip):
        mag, phi = scal[step, 0], scal[step, 1]
        x1 = noise[0, step] * half_root
        x2 = noise[1, step] * half_root
        d = me if which == 0 else j
        z11 = 1.0 - 2.0 * (s & 1)
        z21 = (1 - 2 * ((d >> 3) & 1)).astype(F32)
        place = which * 128 + j * 8 + s
        edge = (couplings[21] * z21) * z0 + energies[place]
        off = pops[place] - mag
        turn = couplings[10] * z11
        grows, spins = [], []
        for u in range(4):
            z10 = -1.0 if u & 2 else 1.0
            shift = occ_base[u] + off
            grows.append(phi * (1.0 + shift * (2.0 * x1 - (DT * KAPPA * 0.5) * shift)))
            energy = en_base[u] + (edge + turn * z10)
            spins.append(phi * ((2.0 * x2) * shift + DT * energy))
        return jnp.stack(grows) * psi + times_i(jnp.stack(spins) * psi + (DT * phi)[None] * flip)

    def weigh(index, psi, carry):
        norm8, mag8 = carry
        weight = psi * psi
        total = jnp.sum(weight, axis=0)
        part = jnp.sum(weight * occ_base[...], axis=0)
        return norm8 + total, mag8 + part + pops[index] * total

    zero8 = jnp.zeros((8, 128), F32)

    def local_flips(src, dst, lo=0, hi=16):
        def one(k, _):
            block = src[k]
            lanes = jnp.dot(
                block.reshape(256, 128), table[...],
                precision=lax.Precision.HIGHEST, preferred_element_type=F32,
            ).reshape(SUBS, 4, 8, 128)
            for s in range(SUBS):
                here = block[s]
                total = lanes[s]
                total = total + fields[7] * jnp.where(
                    bit1_3, pltpu.roll(here, 6, 1), pltpu.roll(here, 2, 1)
                )
                total = total + fields[8] * pltpu.roll(here, 4, 1)
                for b in range(2):
                    total = total + fields[9 + b] * jnp.stack([here[u ^ (1 << b)] for u in range(4)])
                for b in range(3):
                    total = total + fields[11 + b] * block[s ^ (1 << b)]
                for b in range(4):
                    total = total + fields[14 + b] * src[k ^ (1 << b), s]
                dst[k, s] = total
            return 0

        lax.fori_loop(lo, hi, one, 0)

    def high_flip(src, side, d, s):
        total = fields[18] * src[side, d ^ 1, s]
        for b in range(1, 4):
            total = total + fields[18 + b] * src[side, d ^ (1 << b), s]
        return total

    def round_of(r, start, finish):
        base = 4 * r
        first, second = 2 * r, 2 * r + 1
        held, out1, in1, out2, in2 = bp.at[r], v1b.at[r], v1a.at[r], v2b.at[r], v2a.at[r]
        keep_own(start, held)
        for part in range(4):
            for s in range(2 * part, 2 * part + 2):
                wait_group(base, s)
                relay(held, base, s)
            local_flips(start, flips, 4 * part, 4 * part + 4)
        for s in range(SUBS):
            wait_group(base + 1, s, 16)

            def one(d, _):
                for side in range(2):
                    out1[side, d, s] = high_flip(held, side, d, s)
                return 0

            lax.fori_loop(0, 16, one, 0)
            send_back(out1, in1, base + 2, s)
        take_own(out1, in1)
        reduce_wait(first)
        for s in range(SUBS):

            def one(d, _):
                for side in range(2):
                    why[side, d, s] = moved(first, 1 + side, d, s, held[side, d, s], out1[side, d, s])
                return 0

            lax.fori_loop(0, 16, one, 0)

            def two(i, _):
                d = me ^ near_mask(s, i)
                for side in range(2):
                    out2[side, d, s] = high_flip(why, side, d, s)
                return 0

            lax.fori_loop(0, 8, two, 0)
            if s < SUBS // 2:
                send_back(out2, in2, base + 3, s)
        take_own(out2, in2)
        carry = (zero8, zero8)
        for s in range(SUBS):
            wait_group(base + 2, s)

            def one(k, carry):
                back = in1[k, s]
                new = moved(first, 0, k, s, start[k, s], flips[k, s] + back)
                psi1[k, s] = new
                tee[k, s] = new + times_i((DT * scal[first, 1])[None] * back)
                return weigh(k * 8 + s, new, carry)

            carry = lax.fori_loop(0, 16, one, carry)
        reduce_send(second, *carry)
        for s in range(SUBS // 2, SUBS):
            send_back(out2, in2, base + 3, s)
        local_flips(tee, flips)
        reduce_wait(second)
        if r == 0:
            carry = (zero8, zero8)
            for s in range(SUBS):
                wait_group(base + 3, s)

                def one(k, carry):
                    new = moved(second, 0, k, s, psi1[k, s], flips[k, s] + in2[k, s])
                    finish[k, s] = new
                    return weigh(k * 8 + s, new, carry)

                carry = lax.fori_loop(0, 16, one, carry)
                send_direct(finish, bp.at[1], 4, s)
            reduce_send(2, *carry)
        else:
            send_record()
            for s in range(SUBS):

                def one(k, _):
                    psi1[k, s] = moved(second, 0, k, s, psi1[k, s], flips[k, s])
                    return 0

                lax.fori_loop(0, 16, one, 0)
            settle()
            turn = (DT * scal[second, 1])[None]
            for s in range(SUBS):
                wait_group(base + 3, s)

                def one(k, _):
                    finish[k, s] = psi1[k, s] + times_i(turn * in2[k, s])
                    return 0

                lax.fori_loop(0, 16, one, 0)

    def send_record():
        total = zero8
        for step in range(4):
            kick = jnp.where(sub == 0, noise[0, step], noise[1, step]) * half_root
            total = total + jnp.where(lane == step, (KAPPA ** 0.5 * DT) * scal[step, 0] + kick, 0.0)
        rec_src[...] = total
        rec_dst[gy] = total

        def one(k, _):
            pltpu.make_async_remote_copy(
                src_ref=rec_src, dst_ref=rec_dst.at[gy],
                send_sem=rec_send, recv_sem=rec_recv,
                device_id=(me, gy ^ k), device_id_type=MESH,
            ).start()
            return 0

        lax.fori_loop(1, n_gy, one, 0)

    def wait_sent(move):
        for s in range(SUBS):
            count = 16 if move % 4 == 1 else 14
            wait_bytes(bp.at[0, 0, pl.ds(0, count), s], send_sem.at[move, s])

    def settle():
        wait_bytes(rec_dst.at[pl.ds(0, 7)], rec_recv)
        rec_ref[...] = jnp.sum(rec_dst[...], axis=0)[0:2, 0:4]
        for move in range(7):
            wait_sent(move)
        for step in range(4):
            wait_bytes(red_dst.at[step, pl.ds(0, 15)], red_send.at[step])
        wait_bytes(rec_dst.at[pl.ds(0, 7)], rec_send)

    for s in range(SUBS):
        send_direct(x_ref, bp.at[0], 0, s)

    rows = lax.broadcasted_iota(jnp.int32, (128, 128), 0)
    cols = lax.broadcasted_iota(jnp.int32, (128, 128), 1)
    diff = rows ^ cols
    flip_table = jnp.zeros((128, 128), F32)
    for q in range(7):
        flip_table = jnp.where(diff == 1 << q, fields[q], flip_table)
    table[...] = flip_table
    for u in range(4):
        low = lane | ((sub >> 1) << 7) | (u << 9)
        pair = low ^ (low >> 1)
        pop = jnp.zeros((8, 128), jnp.int32)
        energy = jnp.zeros((8, 128), F32)
        for q in range(11):
            pop = pop + ((low >> q) & 1)
        for q in range(10):
            energy = energy + couplings[q] * (1.0 - 2.0 * ((pair >> q) & 1).astype(F32))
        occ_base[u] = pop.astype(F32) * (1.0 / NQ)
        en_base[u] = energy

    def spin(number, bit):
        return (1 - 2 * ((number >> bit) & 1)).astype(F32)

    def fill_parts(i, _):
        pair = i ^ (i >> 1)
        parts[i] = couplings[11] * spin(pair, 0) + couplings[12] * spin(pair, 1)
        for first, at in ((14, 16), (18, 32)):
            total = couplings[first] * spin(pair, 0)
            for b in range(1, 3):
                total = total + couplings[first + b] * spin(pair, b)
            parts[at + i] = total
        count = (i & 1) + ((i >> 1) & 1) + ((i >> 2) & 1) + ((i >> 3) & 1)
        parts[48 + i] = count.astype(F32) * (1.0 / NQ)
        return 0

    lax.fori_loop(0, 16, fill_parts, 0)

    def fill(i, _):
        j, s = i >> 3, i & 7
        for which, k, d in ((0, j, me), (1, me, j), (2, me ^ partner_mask(s), j)):
            energies[which * 128 + i] = (
                parts[s] + parts[16 + k] + parts[32 + d]
                + couplings[13] * spin((s >> 2) ^ k, 0) + couplings[17] * spin((k >> 3) ^ d, 0)
            )
            pops[which * 128 + i] = parts[48 + s] + parts[48 + k] + parts[48 + d]
        return 0

    lax.fori_loop(0, 128, fill, 0)

    def first_weigh(i, carry):
        return weigh(i, x_ref[i >> 3, i & 7], carry)

    reduce_send(0, *lax.fori_loop(0, 128, first_weigh, (zero8, zero8)))
    round_of(0, x_ref, psi2)
    round_of(1, psi2, o_ref)

    wait_sent(7)


def store(final, record, final_hbm, record_hbm, sems):
    first = pltpu.make_async_copy(final, final_hbm, sems.at[0])
    second = pltpu.make_async_copy(record, record_hbm, sems.at[1])
    first.start()
    second.start()
    second.wait()
    first.wait()


def shards(state, fields, couplings, noise):
    block = (16, SUBS, 4, 8, 128)
    x = state.reshape(2, 2048, 128).transpose(1, 0, 2).reshape(block)
    big = pltpu.VMEM(block, F32)
    pair = pltpu.VMEM((2, *block), F32)
    twin = pltpu.VMEM((2, 2, *block), F32)
    smem = pl.BlockSpec(memory_space=pltpu.SMEM)
    vmem = pl.BlockSpec(memory_space=pltpu.VMEM)
    final, record = pl.pallas_call(
        kernel,
        out_shape=(pltpu.VMEM(block, F32), pltpu.VMEM((2, 4), F32)),
        in_specs=[smem, smem, smem, pl.BlockSpec(memory_space=pl.ANY)],
        out_specs=(vmem, vmem),
        scratch_shapes=[
            big, twin, twin, pair, twin, pair, big, big, big, pair, big,
            pltpu.VMEM((128, 128), F32), pltpu.VMEM((4, 8, 128), F32), pltpu.VMEM((4, 8, 128), F32),
            pltpu.VMEM((4, 2, 8, 128), F32), pltpu.VMEM((4, 2, 128), F32), pltpu.VMEM((4, 16, 2, 128), F32),
            pltpu.VMEM((8, 128), F32), pltpu.VMEM((8, 8, 128), F32),
            pltpu.SMEM((64,), F32), pltpu.SMEM((384,), F32), pltpu.SMEM((384,), F32),
            pltpu.SemaphoreType.DMA((8, SUBS)), pltpu.SemaphoreType.DMA((8, SUBS)),
            pltpu.SemaphoreType.DMA((4,)), pltpu.SemaphoreType.DMA((4,)),
            pltpu.SemaphoreType.DMA, pltpu.SemaphoreType.DMA, pltpu.SemaphoreType.DMA,
        ],
        compiler_params=pltpu.CompilerParams(
            collective_id=0, has_side_effects=True, vmem_limit_bytes=60 * 1024 * 1024
        ),
    )(fields, couplings, noise.transpose(0, 2, 1).reshape(2, 4), x)
    hbm = pl.BlockSpec(memory_space=pl.ANY)
    final, record = pl.pallas_call(
        store,
        out_shape=(jax.ShapeDtypeStruct(block, F32), jax.ShapeDtypeStruct((2, 4), F32)),
        in_specs=[vmem, vmem],
        out_specs=(hbm, hbm),
        scratch_shapes=[pltpu.SemaphoreType.DMA((2,))],
        compiler_params=pltpu.CompilerParams(vmem_limit_bytes=256 * 1024),
    )(final, record)
    final = final.reshape(2048, 2, 128).transpose(1, 0, 2).reshape(1, 2, 262144)
    return final, record.transpose(1, 0)


def solution(mesh):
    placed = (P("gy", None, "gx"), P(), P(), P("gy", None, None))
    return jax.shard_map(
        shards, mesh=mesh, in_specs=placed, out_specs=(P("gy", None, "gx"), P()), check_vma=False
    )
```

```python
import functools

import jax
import jax.numpy as jnp
from jax import lax
from jax.experimental import pallas as pl
from jax.experimental.pallas import tpu as pltpu
from jax.sharding import PartitionSpec as P

MESH = pl.DeviceIdType.MESH
KAPPA = 4.0
DT = 0.05
NQ = 22
DIM = 4194304
SUBS = 8
F32 = jnp.float32


def kernel(
    fields, couplings, noise, x_hbm, o_ref, rec_ref,
    x_ref, bp, v1b, v1a, v2b, v2a, psi1, tee, flips, why, psi2,
    table, occ_base, en_base, scal, red_src, red_dst, rec_src, rec_dst, parts, energies, pops,
    send_sem, recv_sem, red_send, red_recv, rec_send, rec_recv, load_sem,
):
    me = lax.axis_index("gx")
    gy = lax.axis_index("gy")
    n_gx, n_gy = 16, 8

    barrier = pltpu.get_barrier_semaphore()

    def greet(k, _):
        pl.semaphore_signal(barrier, inc=1, device_id=(me ^ k, gy), device_id_type=MESH)
        return 0

    def greet_y(k, _):
        pl.semaphore_signal(barrier, inc=1, device_id=(me, gy ^ k), device_id_type=MESH)
        return 0

    load = pltpu.make_async_copy(x_hbm, x_ref, load_sem)
    load.start()
    lax.fori_loop(1, n_gx, greet, 0)
    lax.fori_loop(1, n_gy, greet_y, 0)

    shape3 = (4, 8, 128)
    sub = lax.broadcasted_iota(jnp.int32, (8, 128), 0)
    lane = lax.broadcasted_iota(jnp.int32, (8, 128), 1)
    even = (sub & 1) == 0
    sign = jnp.where(even, -1.0, 1.0).astype(F32)
    bit1 = (sub & 2) == 0
    even3 = jnp.broadcast_to(even[None], shape3)
    bit1_3 = jnp.broadcast_to(bit1[None], shape3)
    z0 = 1.0 - 2.0 * (lane & 1).astype(F32)

    def times_i(y):
        return sign[None] * jnp.where(even3, pltpu.roll(y, 7, 1), pltpu.roll(y, 1, 1))

    load.wait()
    pl.semaphore_wait(barrier, n_gx - 1 + n_gy - 1)

    def partner_mask(s):
        t = s & 3
        return (1 + 2 * (t >> 1)) * (4 - 3 * (t & 1))

    def near_mask(s, i):
        t = s & 3
        return (i >> 2) * (3 - 2 * (t >> 1)) * (4 - 3 * (t & 1)) + (i & 3) * (1 + 3 * (t & 1))

    def start_copy(src, dst, move, s, other):
        pltpu.make_async_remote_copy(
            src_ref=src, dst_ref=dst, send_sem=send_sem.at[move, s], recv_sem=recv_sem.at[move, s],
            device_id=(other, gy), device_id_type=MESH,
        ).start()

    def wait_bytes(ref, sem):
        pltpu.make_async_copy(ref, ref, sem).wait()

    def wait_group(move, s, count=14):
        wait_bytes(bp.at[0, 0, pl.ds(0, count), s], recv_sem.at[move, s])

    def send_direct(src, dst, move, s):
        pm = partner_mask(s)
        partner = me ^ pm

        def one(i, _):
            other = me ^ near_mask(s, i)
            start_copy(src.at[other, s], dst.at[0, me, s], move, s, other)
            start_copy(src.at[other ^ pm, s], dst.at[1, me, s], move, s, other)
            return 0

        lax.fori_loop(1, 8, one, 0)
        start_copy(src.at[partner, s], dst.at[0, me, s], move + 1, s, partner)
        start_copy(src.at[me, s], dst.at[1, me, s], move + 1, s, partner)

    def relay(held, move, s):
        partner = me ^ partner_mask(s)

        def one(i, _):
            source = me ^ near_mask(s, i)
            start_copy(held.at[0, source, s], held.at[1, source, s], move + 1, s, partner)
            start_copy(held.at[1, source, s], held.at[0, source, s], move + 1, s, partner)
            return 0

        lax.fori_loop(1, 8, one, 0)

    def send_back(src, dst, move, s):
        pm = partner_mask(s)

        def one(i, _):
            other = me ^ near_mask(s, i)
            start_copy(src.at[0, other, s], dst.at[me, s], move, s, other)
            start_copy(src.at[1, other, s], dst.at[me ^ pm, s], move, s, other)
            return 0

        lax.fori_loop(1, 8, one, 0)

    def keep_own(src, dst):
        def one(s, _):
            dst[0, me, s] = src[me, s]
            dst[1, me, s] = src[me ^ partner_mask(s), s]
            return 0

        lax.fori_loop(0, SUBS, one, 0)

    def take_own(src, dst):
        def one(s, _):
            dst[me, s] = src[0, me, s]
            dst[me ^ partner_mask(s), s] = src[1, me, s]
            return 0

        lax.fori_loop(0, SUBS, one, 0)

    def reduce_send(step, norm8, mag8):
        norm = jnp.sum(norm8, axis=0, keepdims=True)
        mag = jnp.sum(mag8, axis=0, keepdims=True)
        both = jnp.where(lane[0:1] < 64, norm + pltpu.roll(norm, 64, 1), mag + pltpu.roll(mag, 64, 1))
        red_src[step] = both
        red_dst[step, me] = both

        def one(k, _):
            pltpu.make_async_remote_copy(
                src_ref=red_src.at[step], dst_ref=red_dst.at[step, me],
                send_sem=red_send.at[step], recv_sem=red_recv.at[step],
                device_id=(me ^ k, gy), device_id_type=MESH,
            ).start()
            return 0

        lax.fori_loop(1, n_gx, one, 0)

    def reduce_wait(step):
        wait_bytes(red_dst.at[step, pl.ds(0, 15)], red_recv.at[step])
        total = jnp.sum(red_dst[step], axis=0)
        low = lane[0:1] < 64
        norm = jnp.sum(jnp.where(low, total, 0.0), axis=1, keepdims=True)
        mag = jnp.sum(jnp.where(low, 0.0, total), axis=1, keepdims=True)
        scal[step, 0] = jnp.broadcast_to(mag / norm, (8, 128))
        scal[step, 1] = jnp.broadcast_to(jnp.sqrt(float(DIM) / norm), (8, 128))

    half_root = 0.15811388300841897

    def moved(step, which, j, s, psi, flip):
        mag, phi = scal[step, 0], scal[step, 1]
        x1 = noise[0, step] * half_root
        x2 = noise[1, step] * half_root
        d = me if which == 0 else j
        z11 = 1.0 - 2.0 * (s & 1)
        z21 = (1 - 2 * ((d >> 3) & 1)).astype(F32)
        place = which * 128 + j * 8 + s
        edge = (couplings[21] * z21) * z0 + energies[place]
        off = pops[place] - mag
        turn = couplings[10] * z11
        grows, spins = [], []
        for u in range(4):
            z10 = -1.0 if u & 2 else 1.0
            shift = occ_base[u] + off
            grows.append(phi * (1.0 + shift * (2.0 * x1 - (DT * KAPPA * 0.5) * shift)))
            energy = en_base[u] + (edge + turn * z10)
            spins.append(phi * ((2.0 * x2) * shift + DT * energy))
        return jnp.stack(grows) * psi + times_i(jnp.stack(spins) * psi + (DT * phi)[None] * flip)

    def weigh(index, psi, carry):
        norm8, mag8 = carry
        weight = psi * psi
        total = jnp.sum(weight, axis=0)
        part = jnp.sum(weight * occ_base[...], axis=0)
        return norm8 + total, mag8 + part + pops[index] * total

    zero8 = jnp.zeros((8, 128), F32)

    def local_flips(src, dst, lo=0, hi=16):
        def one(k, _):
            block = src[k]
            lanes = jnp.dot(
                block.reshape(256, 128), table[...],
                precision=lax.Precision.HIGHEST, preferred_element_type=F32,
            ).reshape(SUBS, 4, 8, 128)
            for s in range(SUBS):
                here = block[s]
                total = lanes[s]
                total = total + fields[7] * jnp.where(
                    bit1_3, pltpu.roll(here, 6, 1), pltpu.roll(here, 2, 1)
                )
                total = total + fields[8] * pltpu.roll(here, 4, 1)
                for b in range(2):
                    total = total + fields[9 + b] * jnp.stack([here[u ^ (1 << b)] for u in range(4)])
                for b in range(3):
                    total = total + fields[11 + b] * block[s ^ (1 << b)]
                for b in range(4):
                    total = total + fields[14 + b] * src[k ^ (1 << b), s]
                dst[k, s] = total
            return 0

        lax.fori_loop(lo, hi, one, 0)

    def high_flip(src, side, d, s):
        total = fields[18] * src[side, d ^ 1, s]
        for b in range(1, 4):
            total = total + fields[18 + b] * src[side, d ^ (1 << b), s]
        return total

    def round_of(r, start, finish):
        base = 4 * r
        first, second = 2 * r, 2 * r + 1
        held, out1, in1, out2, in2 = bp.at[r], v1b.at[r], v1a.at[r], v2b.at[r], v2a.at[r]
        keep_own(start, held)
        for part in range(4):
            for s in range(2 * part, 2 * part + 2):
                wait_group(base, s)
                relay(held, base, s)
            local_flips(start, flips, 4 * part, 4 * part + 4)
        for s in range(SUBS):
            wait_group(base + 1, s, 16)

            def one(d, _):
                for side in range(2):
                    out1[side, d, s] = high_flip(held, side, d, s)
                return 0

            lax.fori_loop(0, 16, one, 0)
            send_back(out1, in1, base + 2, s)
        take_own(out1, in1)
        reduce_wait(first)
        for s in range(SUBS):

            def one(d, _):
                for side in range(2):
                    why[side, d, s] = moved(first, 1 + side, d, s, held[side, d, s], out1[side, d, s])
                return 0

            lax.fori_loop(0, 16, one, 0)

            def two(i, _):
                d = me ^ near_mask(s, i)
                for side in range(2):
                    out2[side, d, s] = high_flip(why, side, d, s)
                return 0

            lax.fori_loop(0, 8, two, 0)
            if s < SUBS // 2:
                send_back(out2, in2, base + 3, s)
        take_own(out2, in2)
        carry = (zero8, zero8)
        for s in range(SUBS):
            wait_group(base + 2, s)

            def one(k, carry):
                back = in1[k, s]
                new = moved(first, 0, k, s, start[k, s], flips[k, s] + back)
                psi1[k, s] = new
                tee[k, s] = new + times_i((DT * scal[first, 1])[None] * back)
                return weigh(k * 8 + s, new, carry)

            carry = lax.fori_loop(0, 16, one, carry)
        reduce_send(second, *carry)
        for s in range(SUBS // 2, SUBS):
            send_back(out2, in2, base + 3, s)
        local_flips(tee, flips)
        reduce_wait(second)
        if r == 0:
            carry = (zero8, zero8)
            for s in range(SUBS):
                wait_group(base + 3, s)

                def one(k, carry):
                    new = moved(second, 0, k, s, psi1[k, s], flips[k, s] + in2[k, s])
                    finish[k, s] = new
                    return weigh(k * 8 + s, new, carry)

                carry = lax.fori_loop(0, 16, one, carry)
                send_direct(finish, bp.at[1], 4, s)
            reduce_send(2, *carry)
        else:
            send_record()
            for s in range(SUBS):

                def one(k, _):
                    psi1[k, s] = moved(second, 0, k, s, psi1[k, s], flips[k, s])
                    return 0

                lax.fori_loop(0, 16, one, 0)
            settle()
            turn = (DT * scal[second, 1])[None]
            for s in range(SUBS):
                wait_group(base + 3, s)

                def one(k, _):
                    finish[k, s] = psi1[k, s] + times_i(turn * in2[k, s])
                    return 0

                lax.fori_loop(0, 16, one, 0)

    def send_record():
        total = zero8
        for step in range(4):
            kick = jnp.where(sub == 0, noise[0, step], noise[1, step]) * half_root
            total = total + jnp.where(lane == step, (KAPPA ** 0.5 * DT) * scal[step, 0] + kick, 0.0)
        rec_src[...] = total
        rec_dst[gy] = total

        def one(k, _):
            pltpu.make_async_remote_copy(
                src_ref=rec_src, dst_ref=rec_dst.at[gy],
                send_sem=rec_send, recv_sem=rec_recv,
                device_id=(me, gy ^ k), device_id_type=MESH,
            ).start()
            return 0

        lax.fori_loop(1, n_gy, one, 0)

    def wait_sent(move):
        for s in range(SUBS):
            count = 16 if move % 4 == 1 else 14
            wait_bytes(bp.at[0, 0, pl.ds(0, count), s], send_sem.at[move, s])

    def settle():
        wait_bytes(rec_dst.at[pl.ds(0, 7)], rec_recv)
        rec_ref[...] = jnp.sum(rec_dst[...], axis=0)[0:2, 0:4]
        for move in range(7):
            wait_sent(move)
        for step in range(4):
            wait_bytes(red_dst.at[step, pl.ds(0, 15)], red_send.at[step])
        wait_bytes(rec_dst.at[pl.ds(0, 7)], rec_send)

    for s in range(SUBS):
        send_direct(x_ref, bp.at[0], 0, s)

    rows = lax.broadcasted_iota(jnp.int32, (128, 128), 0)
    cols = lax.broadcasted_iota(jnp.int32, (128, 128), 1)
    diff = rows ^ cols
    flip_table = jnp.zeros((128, 128), F32)
    for q in range(7):
        flip_table = jnp.where(diff == 1 << q, fields[q], flip_table)
    table[...] = flip_table
    for u in range(4):
        low = lane | ((sub >> 1) << 7) | (u << 9)
        pair = low ^ (low >> 1)
        pop = jnp.zeros((8, 128), jnp.int32)
        energy = jnp.zeros((8, 128), F32)
        for q in range(11):
            pop = pop + ((low >> q) & 1)
        for q in range(10):
            energy = energy + couplings[q] * (1.0 - 2.0 * ((pair >> q) & 1).astype(F32))
        occ_base[u] = pop.astype(F32) * (1.0 / NQ)
        en_base[u] = energy

    def spin(number, bit):
        return (1 - 2 * ((number >> bit) & 1)).astype(F32)

    def fill_parts(i, _):
        pair = i ^ (i >> 1)
        parts[i] = couplings[11] * spin(pair, 0) + couplings[12] * spin(pair, 1)
        for first, at in ((14, 16), (18, 32)):
            total = couplings[first] * spin(pair, 0)
            for b in range(1, 3):
                total = total + couplings[first + b] * spin(pair, b)
            parts[at + i] = total
        count = (i & 1) + ((i >> 1) & 1) + ((i >> 2) & 1) + ((i >> 3) & 1)
        parts[48 + i] = count.astype(F32) * (1.0 / NQ)
        return 0

    lax.fori_loop(0, 16, fill_parts, 0)

    def fill(i, _):
        j, s = i >> 3, i & 7
        for which, k, d in ((0, j, me), (1, me, j), (2, me ^ partner_mask(s), j)):
            energies[which * 128 + i] = (
                parts[s] + parts[16 + k] + parts[32 + d]
                + couplings[13] * spin((s >> 2) ^ k, 0) + couplings[17] * spin((k >> 3) ^ d, 0)
            )
            pops[which * 128 + i] = parts[48 + s] + parts[48 + k] + parts[48 + d]
        return 0

    lax.fori_loop(0, 128, fill, 0)

    def first_weigh(i, carry):
        return weigh(i, x_ref[i >> 3, i & 7], carry)

    reduce_send(0, *lax.fori_loop(0, 128, first_weigh, (zero8, zero8)))
    round_of(0, x_ref, psi2)
    round_of(1, psi2, o_ref)

    wait_sent(7)


def store(final, record, final_hbm, record_hbm, sems):
    copies = [pltpu.make_async_copy(record, record_hbm, sems.at[0])]
    for i in range(4):
        rows = pl.ds(4 * i, 4)
        copies.append(pltpu.make_async_copy(final.at[rows], final_hbm.at[rows], sems.at[1 + i]))
    for copy in copies:
        copy.start()
    for copy in copies:
        copy.wait()


def shards(state, fields, couplings, noise):
    block = (16, SUBS, 4, 8, 128)
    x = state.reshape(2, 2048, 128).transpose(1, 0, 2).reshape(block)
    big = pltpu.VMEM(block, F32)
    pair = pltpu.VMEM((2, *block), F32)
    twin = pltpu.VMEM((2, 2, *block), F32)
    smem = pl.BlockSpec(memory_space=pltpu.SMEM)
    vmem = pl.BlockSpec(memory_space=pltpu.VMEM)
    final, record = pl.pallas_call(
        kernel,
        out_shape=(pltpu.VMEM(block, F32), pltpu.VMEM((2, 4), F32)),
        in_specs=[smem, smem, smem, pl.BlockSpec(memory_space=pl.ANY)],
        out_specs=(vmem, vmem),
        scratch_shapes=[
            big, twin, twin, pair, twin, pair, big, big, big, pair, big,
            pltpu.VMEM((128, 128), F32), pltpu.VMEM((4, 8, 128), F32), pltpu.VMEM((4, 8, 128), F32),
            pltpu.VMEM((4, 2, 8, 128), F32), pltpu.VMEM((4, 1, 128), F32), pltpu.VMEM((4, 16, 1, 128), F32),
            pltpu.VMEM((8, 128), F32), pltpu.VMEM((8, 8, 128), F32),
            pltpu.SMEM((64,), F32), pltpu.SMEM((384,), F32), pltpu.SMEM((384,), F32),
            pltpu.SemaphoreType.DMA((8, SUBS)), pltpu.SemaphoreType.DMA((8, SUBS)),
            pltpu.SemaphoreType.DMA((4,)), pltpu.SemaphoreType.DMA((4,)),
            pltpu.SemaphoreType.DMA, pltpu.SemaphoreType.DMA, pltpu.SemaphoreType.DMA,
        ],
        compiler_params=pltpu.CompilerParams(
            collective_id=0, has_side_effects=True, vmem_limit_bytes=60 * 1024 * 1024
        ),
    )(fields, couplings, noise.transpose(0, 2, 1).reshape(2, 4), x)
    hbm = pl.BlockSpec(memory_space=pl.ANY)
    final, record = pl.pallas_call(
        store,
        out_shape=(jax.ShapeDtypeStruct(block, F32), jax.ShapeDtypeStruct((2, 4), F32)),
        in_specs=[vmem, vmem],
        out_specs=(hbm, hbm),
        scratch_shapes=[pltpu.SemaphoreType.DMA((5,))],
        compiler_params=pltpu.CompilerParams(vmem_limit_bytes=256 * 1024),
    )(final, record)
    final = final.reshape(2048, 2, 128).transpose(1, 0, 2).reshape(1, 2, 262144)
    return final, record.transpose(1, 0)


def solution(mesh):
    placed = (P("gy", None, "gx"), P(), P(), P("gy", None, None))
    return jax.shard_map(
        shards, mesh=mesh, in_specs=placed, out_specs=(P("gy", None, "gx"), P()), check_vma=False
    )
```
